512 devices in a mesh: grp: 64 (over y, z_hi, x, core), node: 8 (over z_lo).
Axes of the slice: x: 4, y: 4, z: 16 (z_hi: 2, z_lo: 8; z = z_hi * 8 + z_lo), core: 2. Of those that a mesh axis runs over, the one named last changes fastest.
Arguments:
- grad_out: bfloat16 [24576, 2048], P('grp', 'node'), may hold values from -32 to 32
- gate_prob: float32 [24576], P('grp'), may hold values from 0.05 to 1
- hidden: bfloat16 [24576, 7168], P('grp', 'node'), may hold values from -0.19921875 to 0.19921875
- w_down: bfloat16 [2048, 7168], P(None, 'node'), may hold values from -0.0625 to 0.0625
- slot_counts: int32 [64], P('grp'), may hold values from 0 to 384, as said below
Outputs:
- grad_hidden: bfloat16 [24576, 7168], P('grp', 'node')
- grad_weight: bfloat16 [2048, 7168], P('grp', 'node')
The draws below stay inside these ranges and needn't reach their ends.
Inputs may be any that keep to these rules, and one draw needn't show every extreme that they name: `slot_counts`: each count is a multiple of 128; in every draw some group's count is 384.
All inputs are finite; a program needn't handle non-finite values.
Results may differ from the reference program's by a relative error of at most 0.0057.
Values may be sent and summed in bfloat16 or wider, within the bound.
No kernel may reach another device: no remote copies, remote signals or barrier semaphores. Data moves between devices by JAX's collectives and lax.ppermute only.
A program may use at most 64 MiB of HBM per device.

```python
import math
import jax
import jax.numpy as jnp
from jax import lax

D = 2048
FF = 7168
TILE_ROWS = 128
TILES = 3
CAP = 384
GROUPS = 64
ROWS = 24576


def draw_slot_counts(key, part):
    first_key, second_key, third_key = jax.random.split(key, 3)
    choose_full = jax.random.randint(first_key, (GROUPS,), 0, 4)
    light_tiles = jax.random.randint(second_key, (GROUPS,), 0, TILES // 2 + 1)
    tile_counts = jnp.where(choose_full == 0, TILES, light_tiles)
    full_group = jax.random.randint(third_key, (), 0, GROUPS)
    tile_counts = jnp.where(jnp.arange(GROUPS) == full_group, TILES, tile_counts)
    return (tile_counts * TILE_ROWS).astype(jnp.int32)


def raised(entries, rng, source, target, parts, factor):
    owner, partner = [(jnp.arange(entries.shape[position]) // (entries.shape[position] // parts)).reshape([-1 if axis == position else 1 for axis in range(entries.ndim)]) for position in (source, target)]
    chosen = jax.random.permutation(rng, parts)[partner]
    strong = (owner == chosen) | (owner == (partner + parts // 2) % parts)
    return jnp.where(strong, factor * entries, entries)


def shard_levels(own_key, extent, cuts, low, largest):
    def one(position, blocks):
        heights = jax.random.uniform(jax.random.fold_in(jax.random.fold_in(own_key, 6), position), (blocks,), jnp.float32, low / len(cuts), largest / len(cuts))
        return jnp.repeat(jnp.exp(heights), extent[position] // blocks).reshape((-1,) + (1,) * (len(extent) - position - 1))

    loudness = one(*cuts[0])
    for cut in cuts[1:]:
        loudness = loudness * one(*cut)
    return loudness


def gaussian(own_key, extent, width, most, shards=(), kind=jnp.bfloat16):
    values = width * jax.random.normal(own_key, extent, jnp.float32)
    if shards:
        values = values * shard_levels(own_key, extent, shards, -0.22, 0.18)
    return jnp.clip(values, -most, most).astype(kind)


def noise_with(key, shape, spread, limit, cuts, heavy, kind=jnp.bfloat16):
    array = spread * jax.random.normal(key, shape, jnp.float32)
    if cuts:
        array = array * shard_levels(key, shape, cuts, -0.22, 0.18)
    return jnp.clip(raised(array, jax.random.fold_in(key, 3), *heavy), -limit, limit).astype(kind)


def setup_inputs(seed: int = 0) -> dict:
    splits = jax.random.split(jax.random.key(seed), 6)
    return {
        "grad_out": noise_with(splits[0], (ROWS, D), 2.0, 32.0, ((0, 64), (1, 8)), (0, 1, 64, 4.0)),
        "gate_prob": jnp.clip(jnp.exp(math.log(1.0) - 2.9957323 * jax.random.uniform(splits[1], (ROWS,), jnp.float32) ** shard_levels(splits[1], (ROWS,), ((0, 64),), -0.2, 0.2)), 0.05, 1.0),
        "hidden": gaussian(splits[2], (ROWS, FF), 0.03, 0.19921875, ((0, 64), (1, 8))),
        "w_down": gaussian(splits[3], (D, FF), FF ** -0.5, 0.0625, ((1, 8),)),
        "slot_counts": draw_slot_counts(jax.random.fold_in(splits[5], 71), 0),
    }


def reference(grad_out, gate_prob, hidden, w_down, slot_counts):
    scaled = (gate_prob[:, None] * grad_out.astype(jnp.float32)).astype(jnp.bfloat16)
    slot_index = jnp.arange(ROWS, dtype=jnp.int32)
    group_index = (slot_index // CAP).astype(jnp.int32)
    live_slot = (slot_index % CAP) < slot_counts[group_index]
    masked = jnp.where(live_slot[:, None], scaled, jnp.zeros_like(scaled))
    grad_hidden = jnp.dot(masked, w_down, preferred_element_type=jnp.float32)
    grad_hidden = grad_hidden.astype(jnp.bfloat16)
    slot_blocks = masked.reshape(GROUPS, CAP, D)
    hidden_blocks = hidden.reshape(GROUPS, CAP, FF)

    def add_group(running, blocks):
        group_term = jnp.dot(blocks[0].T, blocks[1], preferred_element_type=jnp.float32)
        rounded = lax.optimization_barrier(group_term.astype(jnp.bfloat16))
        return running + rounded.astype(jnp.float32), None

    running, unused = lax.scan(add_group, jnp.zeros((D, FF), jnp.float32), (slot_blocks, hidden_blocks))
    return grad_hidden, running.astype(jnp.bfloat16)
```

```python
import jax
import jax.numpy as jnp
from jax import lax
from jax.sharding import Mesh, PartitionSpec as P

GRP = ("y", "zh", "x", "core")
RING = (0, 2, 4, 6, 7, 5, 3, 1)
CW = [(RING[i], RING[(i + 1) % 8]) for i in range(8)]
CCW = [(b, a) for a, b in CW]


def gather_features(shard):
    rows, width = shard.shape
    table = jnp.array(RING, jnp.int32)
    place = jnp.argsort(table)[lax.axis_index("node")]
    pieces = [(shard, 0)]
    forward = backward = shard
    for step in range(1, 4):
        forward = lax.ppermute(forward, "node", CW)
        backward = lax.ppermute(backward, "node", CCW)
        pieces += [(forward, -step), (backward, step)]
    half = rows // 2
    last = jnp.concatenate(
        [lax.ppermute(forward[:half], "node", CW), lax.ppermute(backward[half:], "node", CCW)], 0
    )
    pieces.append((last, 4))
    full = jnp.zeros((rows, 8 * width), shard.dtype)
    for piece, shift in pieces:
        owner = table[(place + shift + 8) % 8]
        full = lax.dynamic_update_slice(full, piece, (0, owner * width))
    return full


def body(grad_out, gate_prob, hidden, w_down, slot_counts):
    rows = grad_out.shape[0]
    live = jnp.arange(rows, dtype=jnp.int32) < slot_counts[0]
    scaled = gate_prob[:, None] * grad_out.astype(jnp.float32)
    scaled = jnp.where(live[:, None], scaled, 0.0).astype(jnp.bfloat16)
    full = gather_features(scaled)
    term = lax.dot_general(
        full, hidden, (((0,), (0,)), ((), ())), preferred_element_type=jnp.float32
    ).astype(jnp.bfloat16)
    grad_hidden = jnp.dot(full, w_down, preferred_element_type=jnp.float32).astype(jnp.bfloat16)

    units = hidden.shape[1]
    core, zh = lax.axis_index("core"), lax.axis_index("zh")
    blocks = term.reshape(4, 2, 4, 2, 32, units)
    mine = lax.dynamic_index_in_dim(blocks, core, 3, keepdims=False)
    other = lax.dynamic_index_in_dim(blocks, 1 - core, 3, keepdims=False)
    got = lax.ppermute(other, "core", [(0, 1), (1, 0)])
    pair = (mine.astype(jnp.float32) + got.astype(jnp.float32)).astype(jnp.bfloat16)
    pair = pair.transpose(0, 2, 1, 3, 4).reshape(16, 64, units)
    swapped = lax.all_to_all(pair, ("y", "x"), 0, 0, tiled=True)
    total = jnp.sum(swapped.astype(jnp.float32), axis=0).reshape(2, 32, units)
    keep = lax.dynamic_index_in_dim(total, zh, 0, keepdims=False)
    send = lax.dynamic_index_in_dim(total, 1 - zh, 0, keepdims=False).astype(jnp.bfloat16)
    far = lax.ppermute(send, "zh", [(0, 1), (1, 0)])
    return grad_hidden, (keep + far.astype(jnp.float32)).astype(jnp.bfloat16)


def solution(mesh):
    fine = Mesh(mesh.devices.reshape(4, 2, 4, 2, 8), GRP + ("node",))
    return jax.shard_map(
        body,
        mesh=fine,
        in_specs=(P(GRP, "node"), P(GRP), P(GRP, "node"), P(None, "node"), P(GRP)),
        out_specs=(P(GRP, "node"), P(GRP, "node")),
        check_vma=False,
    )
```

```python
import functools

import jax
import jax.numpy as jnp
import numpy as np
from jax import lax
from jax.experimental import pallas as pl
from jax.experimental.pallas import tpu as pltpu
from jax.sharding import Mesh, PartitionSpec as P


GRP = ("y", "zh", "x", "core")
RING = (0, 2, 4, 6, 7, 5, 3, 1)
CW = [(RING[i], RING[(i + 1) % 8]) for i in range(8)]
CCW = [(b, a) for a, b in CW]
SHIFTS = (0, -1, 1, -2, 2, -3, 3, 4)
ORDER = np.array(
    [[RING[(RING.index(n) + s) % 8] for s in SHIFTS] for n in range(8)], np.int32
)
FIRST = 5


def hidden_kernel(order_ref, pieces_ref, w_ref, out_ref, total_ref):
    step = pl.program_id(0)
    part = jnp.dot(pieces_ref[...], w_ref[...], preferred_element_type=jnp.float32)

    @pl.when(step == 0)
    def _():
        total_ref[...] = part

    @pl.when(step > 0)
    def _():
        total_ref[...] += part

    @pl.when(step == pl.num_programs(0) - 1)
    def _():
        out_ref[...] = total_ref[...].astype(out_ref.dtype)


def hidden_grads(order, pieces, w_down):
    rows, model = pieces.shape
    width, units = model // 8, w_down.shape[1]
    return pl.pallas_call(
        hidden_kernel,
        grid_spec=pltpu.PrefetchScalarGridSpec(
            num_scalar_prefetch=1,
            grid=(8,),
            in_specs=[
                pl.BlockSpec((rows, width), lambda k, order_ref: (0, k)),
                pl.BlockSpec((width, units), lambda k, order_ref: (order_ref[k], 0)),
            ],
            out_specs=pl.BlockSpec((rows, units), lambda k, order_ref: (0, 0)),
            scratch_shapes=[pltpu.VMEM((rows, units), jnp.float32)],
        ),
        out_shape=jax.ShapeDtypeStruct((rows, units), jnp.bfloat16),
        cost_estimate=pl.CostEstimate(
            flops=2 * rows * model * units, bytes_accessed=8_000_000, transcendentals=0
        ),
        compiler_params=pltpu.CompilerParams(vmem_limit_bytes=20 << 20),
        name="hidden_grads",
    )(order, pieces, w_down)


def term_kernel(count, core_ref, mine_ref, theirs_ref, hid_ref, hid_theirs_ref, out_ref, left_ref):
    rows = mine_ref.shape[0]
    line = lax.broadcasted_iota(jnp.int32, (128, 256), 0)
    column = lax.broadcasted_iota(jnp.int32, (128, 256), 1)
    wanted = (
        lax.rem(lax.div(line, 8), 4) * 64
        + core_ref[0] * 32
        + lax.div(line, 32) * 8
        + lax.rem(line, 8)
    )
    pick = jnp.where(column == wanted, 1.0, 0.0).astype(jnp.bfloat16)
    for k in range(count):
        for side, ref in ((0, mine_ref), (1, theirs_ref)):
            turned = lax.dot_general(
                pick,
                ref[:, k * 256 : (k + 1) * 256],
                (((1,), (1,)), ((), ())),
                preferred_element_type=jnp.float32,
            )
            for d in range(16):
                left_ref[
                    d * count * 8 + k * 8 : d * count * 8 + k * 8 + 8,
                    side * rows : (side + 1) * rows,
                ] = turned[d * 8 : d * 8 + 8]
    left = left_ref[...].astype(jnp.bfloat16)
    units = out_ref.shape[1]
    for low in range(0, units, 256):
        high = min(low + 256, units)
        product = jnp.dot(
            left[:, :rows], hid_ref[:, low:high], preferred_element_type=jnp.float32
        ) + jnp.dot(
            left[:, rows:], hid_theirs_ref[:, low:high], preferred_element_type=jnp.float32
        )
        out_ref[:, low:high] = product.astype(out_ref.dtype)


def weight_term(core, mine, theirs, hidden, hidden_theirs):
    rows, units = hidden.shape
    count = mine.shape[1] // 256
    vmem = pl.BlockSpec(memory_space=pltpu.VMEM)
    return pl.pallas_call(
        functools.partial(term_kernel, count),
        in_specs=[pl.BlockSpec(memory_space=pltpu.SMEM)] + [vmem] * 4,
        out_specs=vmem,
        out_shape=jax.ShapeDtypeStruct((count * 128, units), jnp.bfloat16),
        scratch_shapes=[pltpu.VMEM((count * 128, 2 * rows), jnp.float32)],
        cost_estimate=pl.CostEstimate(
            flops=count * 128 * 4 * rows * units,
            bytes_accessed=2 * (2 * rows * (count * 256 + units) + count * 128 * units),
            transcendentals=0,
        ),
        compiler_params=pltpu.CompilerParams(vmem_limit_bytes=20 << 20),
        name="weight_term",
    )(core, mine, theirs, hidden, hidden_theirs)


def sum_kernel(order_ref, first_ref, second_ref, out_ref):
    at = 0
    for ref in (first_ref, second_ref):
        total = ref[0].astype(jnp.float32)
        for d in range(1, 16):
            total += ref[d].astype(jnp.float32)
        for k in range(ref.shape[1] // 8):
            out_ref[order_ref[at]] = total[k * 8 : k * 8 + 8].astype(out_ref.dtype)
            at += 1


def plane_sums(order, first, second):
    units = first.shape[2]
    vmem = pl.BlockSpec(memory_space=pltpu.VMEM)
    return pl.pallas_call(
        sum_kernel,
        in_specs=[pl.BlockSpec(memory_space=pltpu.SMEM), vmem, vmem],
        out_specs=vmem,
        out_shape=jax.ShapeDtypeStruct((8, 8, units), jnp.bfloat16),
        cost_estimate=pl.CostEstimate(
            flops=16 * 64 * units, bytes_accessed=2 * 17 * 64 * units, transcendentals=0
        ),
        compiler_params=pltpu.CompilerParams(vmem_limit_bytes=20 << 20),
        name="plane_sums",
    )(order, first, second)


def body(grad_out, gate_prob, hidden, w_down, slot_counts):
    rows, units = hidden.shape
    order = lax.dynamic_index_in_dim(
        jnp.asarray(ORDER), lax.axis_index("node"), 0, keepdims=False
    )
    core = lax.axis_index("core").reshape(1)
    live = jnp.arange(rows, dtype=jnp.int32) < slot_counts[0]
    scaled = gate_prob[:, None] * grad_out.astype(jnp.float32)
    scaled = jnp.where(live[:, None], scaled, 0.0).astype(jnp.bfloat16)

    def swap(value):
        return lax.ppermute(value, "core", [(0, 1), (1, 0)])

    def scatter(term):
        pieces = term.reshape(16, term.shape[0] // 16, units)
        return lax.all_to_all(pieces, ("y", "x"), 0, 0, tiled=True)

    pieces = [scaled]
    forward = backward = scaled
    for _ in range(1, 4):
        forward = lax.ppermute(forward, "node", CW)
        backward = lax.ppermute(backward, "node", CCW)
        pieces += [forward, backward]
    pieces.append(lax.ppermute(forward, "node", CW))

    hidden_theirs = swap(hidden)
    one = jnp.concatenate(pieces[:FIRST], axis=1)
    one_theirs = swap(one)
    term_one = weight_term(core, one, one_theirs, hidden, hidden_theirs)
    first = scatter(term_one)
    two = jnp.concatenate(pieces[FIRST:], axis=1)
    two_theirs = swap(two)
    term_two = weight_term(core, two, two_theirs, hidden, hidden_theirs)
    second = scatter(term_two)
    sums = plane_sums(order, first, second)
    grad_hidden = hidden_grads(order, jnp.concatenate([one, two], axis=1), w_down)
    halves = lax.all_to_all(sums, ("y", "zh"), 0, 0, tiled=True)
    halves = halves.reshape(4, 2, 8, units)
    grad_weight = halves[:, 0].astype(jnp.float32) + halves[:, 1].astype(jnp.float32)
    return grad_hidden, grad_weight.reshape(32, units).astype(jnp.bfloat16)


def solution(mesh):
    fine = Mesh(mesh.devices.reshape(4, 2, 4, 2, 8), GRP + ("node",))
    return jax.shard_map(
        body,
        mesh=fine,
        in_specs=(P(GRP, "node"), P(GRP), P(GRP, "node"), P(None, "node"), P(GRP)),
        out_specs=(P(GRP, "node"), P(GRP, "node")),
        check_vma=False,
    )
```

```python
import functools

import jax
import jax.numpy as jnp
import numpy as np
from jax import lax
from jax.experimental import pallas as pl
from jax.experimental.pallas import tpu as pltpu
from jax.sharding import Mesh, PartitionSpec as P


GRP = ("y", "zh", "x", "core")
RING = (0, 2, 4, 6, 7, 5, 3, 1)
CW = [(RING[i], RING[(i + 1) % 8]) for i in range(8)]
CCW = [(b, a) for a, b in CW]
SHIFTS = (0, -1, 1, -2, 2, -3, 3, 4)
ORDER = np.array(
    [[RING[(RING.index(n) + s) % 8] for s in SHIFTS] for n in range(8)], np.int32
)


def smem():
    return pl.BlockSpec(memory_space=pltpu.SMEM)


def vmem():
    return pl.BlockSpec(memory_space=pltpu.VMEM)


def anywhere():
    return pl.BlockSpec(memory_space=pl.ANY)


def kernel_call(kernel, scalars, arrays, out_shape, scratch, flops, moved, limit):
    several = isinstance(out_shape, (list, tuple))
    return pl.pallas_call(
        kernel,
        in_specs=[smem() for _ in scalars] + [vmem() for _ in arrays],
        out_specs=[vmem() for _ in out_shape] if several else vmem(),
        out_shape=out_shape,
        scratch_shapes=scratch,
        compiler_params=pltpu.CompilerParams(vmem_limit_bytes=limit << 20),
        cost_estimate=pl.CostEstimate(flops=flops, bytes_accessed=moved, transcendentals=0),
    )(*scalars, *arrays)


def scale_kernel(core_ref, count_ref, gate_ref, grad_ref, own_ref, send_ref):
    line = lax.broadcasted_iota(jnp.int32, (256, 256), 0)
    column = lax.broadcasted_iota(jnp.int32, (256, 256), 1)
    half = lax.div(line, 128)
    side = half + core_ref[0] - 2 * half * core_ref[0]
    wanted = lax.div(lax.rem(line, 128), 32) * 64 + side * 32 + lax.rem(line, 32)
    pick = jnp.where(column == wanted, 1.0, 0.0).astype(jnp.bfloat16)
    turned = lax.dot_general(
        pick, grad_ref[...], (((1,), (1,)), ((), ())), preferred_element_type=jnp.float32
    )
    slot = lax.broadcasted_iota(jnp.int32, turned.shape, 1)
    scaled = jnp.where(slot < count_ref[0], turned * gate_ref[...], 0.0).astype(jnp.bfloat16)
    own_ref[...] = scaled[:128]
    send_ref[...] = scaled[128:]


def scale(core, counts, gate, grad):
    rows = grad.shape[0]
    half = jax.ShapeDtypeStruct((128, rows), jnp.bfloat16)
    return kernel_call(
        scale_kernel, (core, counts), (gate.reshape(1, rows), grad), [half, half], [],
        2 * 256 * 256 * rows, 4 * rows * 256, 8,
    )


def term_kernel(k, order_ref, piece_ref, hid_ref, theirs_ref, *refs):
    term_ref, sent_ref, product_ref, sems = refs[-4:]
    back = pltpu.make_async_copy(
        piece_ref.at[pl.ds(128, 128)], sent_ref.at[pl.ds(k * 128, 128)], sems.at[4]
    )
    back.start()
    units = hid_ref.shape[1]
    own, other = piece_ref[:128, :], piece_ref[128:, :]
    for low in range(0, units, 256):
        high = min(low + 256, units)
        product = jnp.dot(own, hid_ref[:, low:high], preferred_element_type=jnp.float32) + jnp.dot(
            other, theirs_ref[:, low:high], preferred_element_type=jnp.float32
        )
        product_ref[:, low:high] = product.astype(product_ref.dtype)
    owner = order_ref[k]
    copies = []
    for x in range(4):
        block = (lax.div(owner, 2) * 4 + x) * 2 + lax.rem(owner, 2)
        at = pl.multiple_of(block * 32, 32)
        copies.append(
            pltpu.make_async_copy(
                product_ref.at[pl.ds(x * 32, 32)], term_ref.at[pl.ds(at, 32)], sems.at[x]
            )
        )
        copies[-1].start()
    for copy in copies:
        copy.wait()
    back.wait()


def add_term(k, order, piece, hidden, hidden_theirs, state):
    rows, units = hidden.shape
    return pl.pallas_call(
        functools.partial(term_kernel, k),
        in_specs=[smem(), vmem(), vmem(), vmem()] + [anywhere() for _ in state],
        out_specs=[anywhere(), anywhere()],
        out_shape=[
            jax.ShapeDtypeStruct((1024, units), jnp.bfloat16),
            jax.ShapeDtypeStruct((1024, rows), jnp.bfloat16),
        ],
        input_output_aliases={4: 0, 5: 1} if state else {},
        scratch_shapes=[
            pltpu.VMEM((128, units), jnp.bfloat16),
            pltpu.SemaphoreType.DMA((5,)),
        ],
        compiler_params=pltpu.CompilerParams(vmem_limit_bytes=8 << 20),
        cost_estimate=pl.CostEstimate(
            flops=128 * 4 * rows * units,
            bytes_accessed=2 * (2 * rows * units + 128 * (units + 3 * rows)),
            transcendentals=0,
        ),
        name="add_term",
    )(order, piece, hidden, hidden_theirs, *state)


def hidden_kernel(order_ref, core_ref, *refs):
    pieces, (theirs_ref, w_ref, out_ref, full_ref) = refs[:8], refs[8:]
    core = core_ref[0]
    for k, piece_ref in enumerate(pieces):
        base = order_ref[k] * 256
        for x in range(4):
            own = pl.multiple_of(base + x * 64 + core * 32, 32)
            other = pl.multiple_of(base + x * 64 + 32 - core * 32, 32)
            at = k * 128 + x * 32
            full_ref[pl.ds(own, 32), :] = piece_ref[x * 32 : x * 32 + 32, :]
            full_ref[pl.ds(other, 32), :] = theirs_ref[at : at + 32, :]
    full = full_ref[...]
    units = out_ref.shape[1]
    for low in range(0, units, 256):
        high = min(low + 256, units)
        out_ref[:, low:high] = lax.dot_general(
            full, w_ref[:, low:high], (((0,), (0,)), ((), ())), preferred_element_type=jnp.float32
        ).astype(out_ref.dtype)


def hidden_grads(order, core, pieces, theirs, w_down):
    model, units = w_down.shape
    rows = theirs.shape[1]
    return kernel_call(
        hidden_kernel, (order, core), (*pieces, theirs, w_down),
        jax.ShapeDtypeStruct((rows, units), jnp.bfloat16),
        [pltpu.VMEM((model, rows), jnp.bfloat16)],
        2 * rows * model * units, 2 * (2 * rows * model + model * units + rows * units),
        24,
    )


def plane_kernel(zh_ref, in_ref, keep_ref, send_ref):
    zh = zh_ref[0]
    mine = pl.multiple_of(zh * 32, 32)
    theirs = pl.multiple_of(32 - zh * 32, 32)
    keep = in_ref[0, pl.ds(mine, 32), :].astype(jnp.float32)
    send = in_ref[0, pl.ds(theirs, 32), :].astype(jnp.float32)
    for chip in range(1, 16):
        keep += in_ref[chip, pl.ds(mine, 32), :].astype(jnp.float32)
        send += in_ref[chip, pl.ds(theirs, 32), :].astype(jnp.float32)
    keep_ref[...] = keep
    send_ref[...] = send.astype(send_ref.dtype)


def plane_sums(zh, parts):
    units = parts.shape[2]
    return kernel_call(
        plane_kernel, (zh,), (parts,),
        [
            jax.ShapeDtypeStruct((32, units), jnp.float32),
            jax.ShapeDtypeStruct((32, units), jnp.bfloat16),
        ],
        [], 16 * 64 * units, 2 * 18 * 64 * units, 8,
    )


def body(grad_out, gate_prob, hidden, w_down, slot_counts):
    _, units = hidden.shape
    order = lax.dynamic_index_in_dim(
        jnp.asarray(ORDER), lax.axis_index("node"), 0, keepdims=False
    )
    core = lax.axis_index("core").reshape(1)
    zh = lax.axis_index("zh").reshape(1)

    def swap(value):
        return lax.ppermute(value, "core", [(0, 1), (1, 0)])

    own, send = scale(core, slot_counts, gate_prob, grad_out)
    theirs = swap(send)
    shard = jnp.concatenate([own, theirs], axis=0)
    hidden_theirs = swap(hidden)

    pieces = [shard]
    forward = backward = shard
    for _ in range(1, 4):
        forward = lax.ppermute(forward, "node", CW)
        backward = lax.ppermute(backward, "node", CCW)
        pieces += [forward, backward]
    pieces.append(lax.ppermute(forward, "node", CW))

    state = ()
    for k, piece in enumerate(pieces):
        state = add_term(k, order, piece, hidden, hidden_theirs, state)
    term, sent = state
    parts = lax.all_to_all(term.reshape(16, 64, units), ("y", "x"), 0, 0, tiled=True)
    theirs = swap(sent)
    grad_hidden = hidden_grads(order, core, pieces, theirs, w_down)
    keep, cross = plane_sums(zh, parts)
    far = lax.ppermute(cross, "zh", [(0, 1), (1, 0)])
    return grad_hidden, (keep + far.astype(jnp.float32)).astype(jnp.bfloat16)


def solution(mesh):
    fine = Mesh(mesh.devices.reshape(4, 2, 4, 2, 8), GRP + ("node",))
    return jax.shard_map(
        body,
        mesh=fine,
        in_specs=(P(GRP, "node"), P(GRP), P(GRP, "node"), P(None, "node"), P(GRP)),
        out_specs=(P(GRP, "node"), P(GRP, "node")),
        check_vma=False,
    )
```

```python
import functools

import jax
import jax.numpy as jnp
import numpy as np
from jax import lax
from jax.experimental import pallas as pl
from jax.experimental.pallas import tpu as pltpu
from jax.sharding import Mesh, PartitionSpec as P


GRP = ("y", "zh", "x", "core")
RING = (0, 2, 4, 6, 7, 5, 3, 1)
CW = [(RING[i], RING[(i + 1) % 8]) for i in range(8)]
CCW = [(b, a) for a, b in CW]
SHIFTS = (0, -1, 1, -2, 2, -3, 3, 4)
ORDER = np.array(
    [[RING[(RING.index(n) + s) % 8] for s in SHIFTS] for n in range(8)], np.int32
)


def smem():
    return pl.BlockSpec(memory_space=pltpu.SMEM)


def vmem():
    return pl.BlockSpec(memory_space=pltpu.VMEM)


def anywhere():
    return pl.BlockSpec(memory_space=pl.ANY)


def kernel_call(kernel, scalars, arrays, out_shape, scratch, flops, moved, limit):
    several = isinstance(out_shape, (list, tuple))
    return pl.pallas_call(
        kernel,
        in_specs=[smem() for _ in scalars] + [vmem() for _ in arrays],
        out_specs=[vmem() for _ in out_shape] if several else vmem(),
        out_shape=out_shape,
        scratch_shapes=scratch,
        compiler_params=pltpu.CompilerParams(vmem_limit_bytes=limit << 20),
        cost_estimate=pl.CostEstimate(flops=flops, bytes_accessed=moved, transcendentals=0),
    )(*scalars, *arrays)


def scale_kernel(count_ref, gate_ref, grad_ref, own_ref, send_ref):
    line = lax.broadcasted_iota(jnp.int32, (256, 256), 0)
    column = lax.broadcasted_iota(jnp.int32, (256, 256), 1)
    half = lax.div(line, 128)
    core = lax.axis_index("core")
    side = half + core - 2 * half * core
    wanted = lax.div(lax.rem(line, 128), 32) * 64 + side * 32 + lax.rem(line, 32)
    pick = jnp.where(column == wanted, 1.0, 0.0).astype(jnp.bfloat16)
    turned = lax.dot_general(
        pick, grad_ref[...], (((1,), (1,)), ((), ())), preferred_element_type=jnp.float32
    )
    slot = lax.broadcasted_iota(jnp.int32, turned.shape, 1)
    scaled = jnp.where(slot < count_ref[0], turned * gate_ref[...][None, :], 0.0).astype(jnp.bfloat16)
    own_ref[...] = scaled[:128]
    send_ref[...] = scaled[128:]


def scale(counts, gate, grad):
    rows = grad.shape[0]
    half = jax.ShapeDtypeStruct((128, rows), jnp.bfloat16)
    return kernel_call(
        scale_kernel, (counts,), (gate, grad), [half, half], [],
        2 * 256 * 256 * rows, 4 * rows * 256, 8,
    )


def join_kernel(own_ref, theirs_ref, out_ref):
    out_ref[:128, :] = own_ref[...]
    out_ref[128:, :] = theirs_ref[...]


def join(own, theirs):
    rows = own.shape[1]
    return kernel_call(
        join_kernel, (), (own, theirs), jax.ShapeDtypeStruct((256, rows), jnp.bfloat16), [],
        0, 4 * 256 * rows, 8,
    )


def term_kernel(k, order_ref, piece_ref, hid_ref, theirs_ref, *refs):
    term_ref, sent_ref, product_ref, sems = refs[-4:]
    back = pltpu.make_async_copy(
        piece_ref.at[pl.ds(128, 128)], sent_ref.at[pl.ds(k * 128, 128)], sems.at[4]
    )
    back.start()
    units = hid_ref.shape[1]
    own, other = piece_ref[:128, :], piece_ref[128:, :]
    for low in range(0, units, 256):
        high = min(low + 256, units)
        product = jnp.dot(own, hid_ref[:, low:high], preferred_element_type=jnp.float32) + jnp.dot(
            other, theirs_ref[:, low:high], preferred_element_type=jnp.float32
        )
        product_ref[:, low:high] = product.astype(product_ref.dtype)
    owner = order_ref[k]
    copies = []
    for x in range(4):
        block = (lax.div(owner, 2) * 4 + x) * 2 + lax.rem(owner, 2)
        at = pl.multiple_of(block * 32, 32)
        copies.append(
            pltpu.make_async_copy(
                product_ref.at[pl.ds(x * 32, 32)], term_ref.at[pl.ds(at, 32)], sems.at[x]
            )
        )
        copies[-1].start()
    for copy in copies:
        copy.wait()
    back.wait()


def add_term(k, order, piece, hidden, hidden_theirs, state):
    rows, units = hidden.shape
    return pl.pallas_call(
        functools.partial(term_kernel, k),
        in_specs=[smem(), vmem(), vmem(), vmem()] + [anywhere() for _ in state],
        out_specs=[anywhere(), anywhere()],
        out_shape=[
            jax.ShapeDtypeStruct((1024, units), jnp.bfloat16),
            jax.ShapeDtypeStruct((1024, rows), jnp.bfloat16),
        ],
        input_output_aliases={4: 0, 5: 1} if state else {},
        scratch_shapes=[
            pltpu.VMEM((128, units), jnp.bfloat16),
            pltpu.SemaphoreType.DMA((5,)),
        ],
        compiler_params=pltpu.CompilerParams(vmem_limit_bytes=8 << 20),
        cost_estimate=pl.CostEstimate(
            flops=128 * 4 * rows * units,
            bytes_accessed=2 * (2 * rows * units + 128 * (units + 3 * rows)),
            transcendentals=0,
        ),
        name="add_term",
    )(order, piece, hidden, hidden_theirs, *state)


def hidden_kernel(order_ref, core_ref, *refs):
    pieces, (theirs_ref, w_ref, out_ref, full_ref) = refs[:8], refs[8:]
    core = core_ref[0]
    for k, piece_ref in enumerate(pieces):
        base = order_ref[k] * 256
        for x in range(4):
            own = pl.multiple_of(base + x * 64 + core * 32, 32)
            other = pl.multiple_of(base + x * 64 + 32 - core * 32, 32)
            at = k * 128 + x * 32
            full_ref[pl.ds(own, 32), :] = piece_ref[x * 32 : x * 32 + 32, :]
            full_ref[pl.ds(other, 32), :] = theirs_ref[at : at + 32, :]
    full = full_ref[...]
    units = out_ref.shape[1]
    for low in range(0, units, 256):
        high = min(low + 256, units)
        out_ref[:, low:high] = lax.dot_general(
            full, w_ref[:, low:high], (((0,), (0,)), ((), ())), preferred_element_type=jnp.float32
        ).astype(out_ref.dtype)


def hidden_grads(order, core, pieces, theirs, w_down):
    model, units = w_down.shape
    rows = theirs.shape[1]
    return kernel_call(
        hidden_kernel, (order, core), (*pieces, theirs, w_down),
        jax.ShapeDtypeStruct((rows, units), jnp.bfloat16),
        [pltpu.VMEM((model, rows), jnp.bfloat16)],
        2 * rows * model * units, 2 * (2 * rows * model + model * units + rows * units),
        24,
    )


def plane_kernel(zh_ref, in_ref, keep_ref, send_ref):
    zh = zh_ref[0]
    mine = pl.multiple_of(zh * 32, 32)
    theirs = pl.multiple_of(32 - zh * 32, 32)
    keep = in_ref[0, pl.ds(mine, 32), :].astype(jnp.float32)
    send = in_ref[0, pl.ds(theirs, 32), :].astype(jnp.float32)
    for chip in range(1, 16):
        keep += in_ref[chip, pl.ds(mine, 32), :].astype(jnp.float32)
        send += in_ref[chip, pl.ds(theirs, 32), :].astype(jnp.float32)
    keep_ref[...] = keep
    send_ref[...] = send.astype(send_ref.dtype)


def plane_sums(zh, parts):
    units = parts.shape[2]
    return kernel_call(
        plane_kernel, (zh,), (parts,),
        [
            jax.ShapeDtypeStruct((32, units), jnp.float32),
            jax.ShapeDtypeStruct((32, units), jnp.bfloat16),
        ],
        [], 16 * 64 * units, 2 * 18 * 64 * units, 8,
    )


def body(grad_out, gate_prob, hidden, w_down, slot_counts):
    _, units = hidden.shape
    order = lax.dynamic_index_in_dim(
        jnp.asarray(ORDER), lax.axis_index("node"), 0, keepdims=False
    )
    core = lax.axis_index("core").reshape(1)
    zh = lax.axis_index("zh").reshape(1)

    def swap(value):
        return lax.ppermute(value, "core", [(0, 1), (1, 0)])

    own, send = scale(slot_counts, gate_prob, grad_out)
    theirs = swap(send)
    shard = join(own, theirs)
    hidden_theirs = swap(hidden)

    pieces = [shard]
    forward = backward = shard
    for _ in range(1, 4):
        forward = lax.ppermute(forward, "node", CW)
        backward = lax.ppermute(backward, "node", CCW)
        pieces += [forward, backward]
    pieces.append(lax.ppermute(forward, "node", CW))

    state = ()
    for k, piece in enumerate(pieces):
        state = add_term(k, order, piece, hidden, hidden_theirs, state)
    term, sent = state
    parts = lax.all_to_all(term.reshape(16, 64, units), ("y", "x"), 0, 0, tiled=True)
    theirs = swap(sent)
    grad_hidden = hidden_grads(order, core, pieces, theirs, w_down)
    keep, cross = plane_sums(zh, parts)
    far = lax.ppermute(cross, "zh", [(0, 1), (1, 0)])
    return grad_hidden, (keep + far.astype(jnp.float32)).astype(jnp.bfloat16)


def solution(mesh):
    fine = Mesh(mesh.devices.reshape(4, 2, 4, 2, 8), GRP + ("node",))
    return jax.shard_map(
        body,
        mesh=fine,
        in_specs=(P(GRP, "node"), P(GRP), P(GRP, "node"), P(None, "node"), P(GRP)),
        out_specs=(P(GRP, "node"), P(GRP, "node")),
        check_vma=False,
    )
```

```python
import functools

import jax
import jax.numpy as jnp
import numpy as np
from jax import lax
from jax.experimental import pallas as pl
from jax.experimental.pallas import tpu as pltpu
from jax.sharding import Mesh, PartitionSpec as P


GRP = ("y", "zh", "x", "core")
RING = (0, 2, 4, 6, 7, 5, 3, 1)
CW = [(RING[(i + 1) % 8], RING[i]) for i in range(8)]
CCW = [(b, a) for a, b in CW]
SHIFTS = (0, 1, -1, 2, -2, 3, -3, 4)
ORDER = np.array(
    [[RING[(RING.index(n) + s) % 8] for s in SHIFTS] for n in range(8)], np.int32
)


def smem():
    return pl.BlockSpec(memory_space=pltpu.SMEM)


def vmem():
    return pl.BlockSpec(memory_space=pltpu.VMEM)


def anywhere():
    return pl.BlockSpec(memory_space=pl.ANY)


def kernel_call(kernel, scalars, arrays, out_shape, scratch, flops, moved, limit):
    several = isinstance(out_shape, (list, tuple))
    return pl.pallas_call(
        kernel,
        in_specs=[smem() for _ in scalars] + [vmem() for _ in arrays],
        out_specs=[vmem() for _ in out_shape] if several else vmem(),
        out_shape=out_shape,
        scratch_shapes=scratch,
        compiler_params=pltpu.CompilerParams(vmem_limit_bytes=limit << 20),
        cost_estimate=pl.CostEstimate(flops=flops, bytes_accessed=moved, transcendentals=0),
    )(*scalars, *arrays)


def scale_kernel(count_ref, gate_ref, grad_ref, own_ref, send_ref):
    line = lax.broadcasted_iota(jnp.int32, (256, 256), 0)
    column = lax.broadcasted_iota(jnp.int32, (256, 256), 1)
    half = lax.div(line, 128)
    core = lax.axis_index("core")
    side = half + core - 2 * half * core
    wanted = lax.div(lax.rem(line, 128), 32) * 64 + side * 32 + lax.rem(line, 32)
    pick = jnp.where(column == wanted, 1.0, 0.0).astype(jnp.bfloat16)
    turned = lax.dot_general(
        pick, grad_ref[...], (((1,), (1,)), ((), ())), preferred_element_type=jnp.float32
    )
    slot = lax.broadcasted_iota(jnp.int32, turned.shape, 1)
    scaled = jnp.where(slot < count_ref[0], turned * gate_ref[...][None, :], 0.0).astype(jnp.bfloat16)
    own_ref[...] = scaled[:128]
    send_ref[...] = scaled[128:]


def scale(counts, gate, grad):
    rows = grad.shape[0]
    half = jax.ShapeDtypeStruct((128, rows), jnp.bfloat16)
    return kernel_call(
        scale_kernel, (counts,), (gate, grad), [half, half], [],
        2 * 256 * 256 * rows, 4 * rows * 256, 8,
    )


def join_kernel(own_ref, theirs_ref, out_ref):
    out_ref[:128, :] = own_ref[...]
    out_ref[128:, :] = theirs_ref[...]


def join(own, theirs):
    rows = own.shape[1]
    return kernel_call(
        join_kernel, (), (own, theirs), jax.ShapeDtypeStruct((256, rows), jnp.bfloat16), [],
        0, 4 * 256 * rows, 8,
    )


def term_kernel(k, order_ref, piece_ref, hid_ref, theirs_ref, *refs):
    term_ref, sent_ref, product_ref, sems = refs[-4:]
    back = pltpu.make_async_copy(
        piece_ref.at[pl.ds(128, 128)], sent_ref.at[pl.ds(k * 128, 128)], sems.at[4]
    )
    back.start()
    units = hid_ref.shape[1]
    own, other = piece_ref[:128, :], piece_ref[128:, :]
    for low in range(0, units, 256):
        high = min(low + 256, units)
        product = jnp.dot(own, hid_ref[:, low:high], preferred_element_type=jnp.float32) + jnp.dot(
            other, theirs_ref[:, low:high], preferred_element_type=jnp.float32
        )
        product_ref[:, low:high] = product.astype(product_ref.dtype)
    owner = order_ref[k]
    copies = []
    for x in range(4):
        block = (x * 4 + lax.div(owner, 2)) * 2 + lax.rem(owner, 2)
        at = pl.multiple_of(block * 32, 32)
        copies.append(
            pltpu.make_async_copy(
                product_ref.at[pl.ds(x * 32, 32)], term_ref.at[pl.ds(at, 32)], sems.at[x]
            )
        )
        copies[-1].start()
    for copy in copies:
        copy.wait()
    back.wait()


def add_term(k, order, piece, hidden, hidden_theirs, state):
    rows, units = hidden.shape
    return pl.pallas_call(
        functools.partial(term_kernel, k),
        in_specs=[smem(), vmem(), vmem(), vmem()] + [anywhere() for _ in state],
        out_specs=[anywhere(), anywhere()],
        out_shape=[
            jax.ShapeDtypeStruct((1024, units), jnp.bfloat16),
            jax.ShapeDtypeStruct((1024, rows), jnp.bfloat16),
        ],
        input_output_aliases={4: 0, 5: 1} if state else {},
        scratch_shapes=[
            pltpu.VMEM((128, units), jnp.bfloat16),
            pltpu.SemaphoreType.DMA((5,)),
        ],
        compiler_params=pltpu.CompilerParams(vmem_limit_bytes=8 << 20),
        cost_estimate=pl.CostEstimate(
            flops=128 * 4 * rows * units,
            bytes_accessed=2 * (2 * rows * units + 128 * (units + 3 * rows)),
            transcendentals=0,
        ),
        name="add_term",
    )(order, piece, hidden, hidden_theirs, *state)


def hidden_kernel(order_ref, core_ref, *refs):
    pieces, (theirs_ref, w_ref, out_ref, full_ref) = refs[:8], refs[8:]
    core = core_ref[0]
    for k, piece_ref in enumerate(pieces):
        base = order_ref[k] * 256
        for x in range(4):
            own = pl.multiple_of(base + x * 64 + core * 32, 32)
            other = pl.multiple_of(base + x * 64 + 32 - core * 32, 32)
            at = k * 128 + x * 32
            full_ref[pl.ds(own, 32), :] = piece_ref[x * 32 : x * 32 + 32, :]
            full_ref[pl.ds(other, 32), :] = theirs_ref[at : at + 32, :]
    full = full_ref[...]
    units = out_ref.shape[1]
    for low in range(0, units, 256):
        high = min(low + 256, units)
        out_ref[:, low:high] = lax.dot_general(
            full, w_ref[:, low:high], (((0,), (0,)), ((), ())), preferred_element_type=jnp.float32
        ).astype(out_ref.dtype)


def hidden_grads(order, core, pieces, theirs, w_down):
    model, units = w_down.shape
    rows = theirs.shape[1]
    return kernel_call(
        hidden_kernel, (order, core), (*pieces, theirs, w_down),
        jax.ShapeDtypeStruct((rows, units), jnp.bfloat16),
        [pltpu.VMEM((model, rows), jnp.bfloat16)],
        2 * rows * model * units, 2 * (2 * rows * model + model * units + rows * units),
        24,
    )


def plane_kernel(zh_ref, in_ref, keep_ref, send_ref):
    zh = zh_ref[0]
    mine = pl.multiple_of(zh * 32, 32)
    theirs = pl.multiple_of(32 - zh * 32, 32)
    keep = in_ref[0, pl.ds(mine, 32), :].astype(jnp.float32)
    send = in_ref[0, pl.ds(theirs, 32), :].astype(jnp.float32)
    for chip in range(1, 16):
        keep += in_ref[chip, pl.ds(mine, 32), :].astype(jnp.float32)
        send += in_ref[chip, pl.ds(theirs, 32), :].astype(jnp.float32)
    keep_ref[...] = keep
    send_ref[...] = send.astype(send_ref.dtype)


def plane_sums(zh, parts):
    units = parts.shape[2]
    return kernel_call(
        plane_kernel, (zh,), (parts,),
        [
            jax.ShapeDtypeStruct((32, units), jnp.float32),
            jax.ShapeDtypeStruct((32, units), jnp.bfloat16),
        ],
        [], 16 * 64 * units, 2 * 18 * 64 * units, 8,
    )


def body(grad_out, gate_prob, hidden, w_down, slot_counts):
    _, units = hidden.shape
    order = lax.dynamic_index_in_dim(
        jnp.asarray(ORDER), lax.axis_index("node"), 0, keepdims=False
    )
    core = lax.axis_index("core").reshape(1)
    zh = lax.axis_index("zh").reshape(1)

    def swap(value):
        return lax.ppermute(value, "core", [(0, 1), (1, 0)])

    own, send = scale(slot_counts, gate_prob, grad_out)
    theirs = swap(send)
    shard = join(own, theirs)
    hidden_theirs = swap(hidden)

    pieces = [shard]
    forward = backward = shard
    for _ in range(1, 4):
        forward = lax.ppermute(forward, "node", CW)
        backward = lax.ppermute(backward, "node", CCW)
        pieces += [forward, backward]
    pieces.append(lax.ppermute(forward, "node", CW))

    state = ()
    for k, piece in enumerate(pieces):
        state = add_term(k, order, piece, hidden, hidden_theirs, state)
    term, sent = state
    parts = lax.all_to_all(term.reshape(16, 64, units), ("x", "y"), 0, 0, tiled=True)
    theirs = swap(sent)
    grad_hidden = hidden_grads(order, core, pieces, theirs, w_down)
    keep, cross = plane_sums(zh, parts)
    far = lax.ppermute(cross, "zh", [(0, 1), (1, 0)])
    return grad_hidden, (keep + far.astype(jnp.float32)).astype(jnp.bfloat16)


def solution(mesh):
    fine = Mesh(mesh.devices.reshape(4, 2, 4, 2, 8), GRP + ("node",))
    return jax.shard_map(
        body,
        mesh=fine,
        in_specs=(P(GRP, "node"), P(GRP), P(GRP, "node"), P(None, "node"), P(GRP)),
        out_specs=(P(GRP, "node"), P(GRP, "node")),
        check_vma=False,
    )
```

```python
import functools

import jax
import jax.numpy as jnp
import numpy as np
from jax import lax
from jax.experimental import pallas as pl
from jax.experimental.pallas import tpu as pltpu
from jax.sharding import Mesh, PartitionSpec as P


GRP = ("y", "zh", "x", "core")
RING = (0, 2, 4, 6, 7, 5, 3, 1)
CW = [(RING[(i + 1) % 8], RING[i]) for i in range(8)]
CCW = [(b, a) for a, b in CW]
SHIFTS = (0, 1, -1, 2, -2, 3, -3, 4)
ORDER = np.array(
    [[RING[(RING.index(n) + s) % 8] for s in SHIFTS] for n in range(8)], np.int32
)


def smem():
    return pl.BlockSpec(memory_space=pltpu.SMEM)


def vmem():
    return pl.BlockSpec(memory_space=pltpu.VMEM)


def anywhere():
    return pl.BlockSpec(memory_space=pl.ANY)


def kernel_call(kernel, scalars, arrays, out_shape, scratch, flops, moved, limit):
    several = isinstance(out_shape, (list, tuple))
    return pl.pallas_call(
        kernel,
        in_specs=[smem() for _ in scalars] + [vmem() for _ in arrays],
        out_specs=[vmem() for _ in out_shape] if several else vmem(),
        out_shape=out_shape,
        scratch_shapes=scratch,
        compiler_params=pltpu.CompilerParams(vmem_limit_bytes=limit << 20),
        cost_estimate=pl.CostEstimate(flops=flops, bytes_accessed=moved, transcendentals=0),
    )(*scalars, *arrays)


def scale_kernel(count_ref, gate_ref, grad_ref, own_ref, send_ref):
    line = lax.broadcasted_iota(jnp.int32, (256, 256), 0)
    column = lax.broadcasted_iota(jnp.int32, (256, 256), 1)
    half = lax.div(line, 128)
    core = lax.axis_index("core")
    side = half + core - 2 * half * core
    wanted = lax.div(lax.rem(line, 128), 32) * 64 + side * 32 + lax.rem(line, 32)
    pick = jnp.where(column == wanted, 1.0, 0.0).astype(jnp.bfloat16)
    turned = lax.dot_general(
        pick, grad_ref[...], (((1,), (1,)), ((), ())), preferred_element_type=jnp.float32
    )
    slot = lax.broadcasted_iota(jnp.int32, turned.shape, 1)
    scaled = jnp.where(slot < count_ref[0], turned * gate_ref[...][None, :], 0.0).astype(jnp.bfloat16)
    own_ref[...] = scaled[:128]
    send_ref[...] = scaled[128:]


def scale(counts, gate, grad):
    rows = grad.shape[0]
    half = jax.ShapeDtypeStruct((128, rows), jnp.bfloat16)
    return kernel_call(
        scale_kernel, (counts,), (gate, grad), [half, half], [],
        2 * 256 * 256 * rows, 4 * rows * 256, 8,
    )


def join_kernel(own_ref, theirs_ref, out_ref):
    out_ref[:128, :] = own_ref[...]
    out_ref[128:, :] = theirs_ref[...]


def join(own, theirs):
    rows = own.shape[1]
    return kernel_call(
        join_kernel, (), (own, theirs), jax.ShapeDtypeStruct((256, rows), jnp.bfloat16), [],
        0, 4 * 256 * rows, 8,
    )


def term_kernel(k, order_ref, piece_ref, hid_ref, theirs_ref, *refs):
    term_ref, sent_ref, product_ref, sems = refs[-4:]
    back = pltpu.make_async_copy(
        piece_ref.at[pl.ds(128, 128)], sent_ref.at[pl.ds(k * 128, 128)], sems.at[4]
    )
    back.start()
    units = hid_ref.shape[1]
    own, other = piece_ref[:128, :], piece_ref[128:, :]
    for low in range(0, units, 256):
        high = min(low + 256, units)
        product = jnp.dot(own, hid_ref[:, low:high], preferred_element_type=jnp.float32) + jnp.dot(
            other, theirs_ref[:, low:high], preferred_element_type=jnp.float32
        )
        product_ref[:, low:high] = product.astype(product_ref.dtype)
    owner = order_ref[k]
    copies = []
    for x in range(4):
        block = (x * 4 + lax.div(owner, 2)) * 2 + lax.rem(owner, 2)
        at = pl.multiple_of(block * 32, 32)
        copies.append(
            pltpu.make_async_copy(
                product_ref.at[pl.ds(x * 32, 32)], term_ref.at[pl.ds(at, 32)], sems.at[x]
            )
        )
        copies[-1].start()
    for copy in copies:
        copy.wait()
    back.wait()


def add_term(k, order, piece, hidden, hidden_theirs, state):
    rows, units = hidden.shape
    return pl.pallas_call(
        functools.partial(term_kernel, k),
        in_specs=[smem(), vmem(), vmem(), vmem()] + [anywhere() for _ in state],
        out_specs=[anywhere(), anywhere()],
        out_shape=[
            jax.ShapeDtypeStruct((1024, units), jnp.bfloat16),
            jax.ShapeDtypeStruct((1024, rows), jnp.bfloat16),
        ],
        input_output_aliases={4: 0, 5: 1} if state else {},
        scratch_shapes=[
            pltpu.VMEM((128, units), jnp.bfloat16),
            pltpu.SemaphoreType.DMA((5,)),
        ],
        compiler_params=pltpu.CompilerParams(vmem_limit_bytes=8 << 20),
        cost_estimate=pl.CostEstimate(
            flops=128 * 4 * rows * units,
            bytes_accessed=2 * (2 * rows * units + 128 * (units + 3 * rows)),
            transcendentals=0,
        ),
        name="add_term",
    )(order, piece, hidden, hidden_theirs, *state)


def hidden_kernel(order_ref, core_ref, *refs):
    pieces, (theirs_ref, w_ref, out_ref, full_ref) = refs[:8], refs[8:]
    core = core_ref[0]
    for k, piece_ref in enumerate(pieces):
        base = order_ref[k] * 256
        for x in range(4):
            own = pl.multiple_of(base + x * 64 + core * 32, 32)
            other = pl.multiple_of(base + x * 64 + 32 - core * 32, 32)
            at = k * 128 + x * 32
            full_ref[pl.ds(own, 32), :] = piece_ref[x * 32 : x * 32 + 32, :]
            full_ref[pl.ds(other, 32), :] = theirs_ref[at : at + 32, :]
    full = full_ref[...]
    units = out_ref.shape[1]
    for low in range(0, units, 256):
        high = min(low + 256, units)
        out_ref[:, low:high] = lax.dot_general(
            full, w_ref[:, low:high], (((0,), (0,)), ((), ())), preferred_element_type=jnp.float32
        ).astype(out_ref.dtype)


def hidden_grads(order, core, pieces, theirs, w_down):
    model, units = w_down.shape
    rows = theirs.shape[1]
    return kernel_call(
        hidden_kernel, (order, core), (*pieces, theirs, w_down),
        jax.ShapeDtypeStruct((rows, units), jnp.bfloat16),
        [pltpu.VMEM((model, rows), jnp.bfloat16)],
        2 * rows * model * units, 2 * (2 * rows * model + model * units + rows * units),
        24,
    )


def plane_kernel(zh_ref, in_ref, keep_ref, send_ref):
    zh = zh_ref[0]
    mine = pl.multiple_of(zh * 32, 32)
    theirs = pl.multiple_of(32 - zh * 32, 32)
    keep = in_ref[0, pl.ds(mine, 32), :].astype(jnp.float32)
    send = in_ref[0, pl.ds(theirs, 32), :].astype(jnp.float32)
    for chip in range(1, 16):
        keep += in_ref[chip, pl.ds(mine, 32), :].astype(jnp.float32)
        send += in_ref[chip, pl.ds(theirs, 32), :].astype(jnp.float32)
    keep_ref[...] = keep
    send_ref[...] = send.astype(send_ref.dtype)


def plane_sums(zh, parts):
    units = parts.shape[2]
    return kernel_call(
        plane_kernel, (zh,), (parts,),
        [
            jax.ShapeDtypeStruct((32, units), jnp.float32),
            jax.ShapeDtypeStruct((32, units), jnp.bfloat16),
        ],
        [], 16 * 64 * units, 2 * 18 * 64 * units, 8,
    )


def finish_kernel(keep_ref, far_ref, out_ref):
    out_ref[...] = (keep_ref[...] + far_ref[...].astype(jnp.float32)).astype(out_ref.dtype)


def finish(keep, far):
    return kernel_call(
        finish_kernel, (), (keep, far), jax.ShapeDtypeStruct(far.shape, jnp.bfloat16), [],
        keep.size, 8 * keep.size, 4,
    )


def body(grad_out, gate_prob, hidden, w_down, slot_counts):
    _, units = hidden.shape
    order = lax.dynamic_index_in_dim(
        jnp.asarray(ORDER), lax.axis_index("node"), 0, keepdims=False
    )
    core = lax.axis_index("core").reshape(1)
    zh = lax.axis_index("zh").reshape(1)

    def swap(value):
        return lax.ppermute(value, "core", [(0, 1), (1, 0)])

    own, send = scale(slot_counts, gate_prob, grad_out)
    theirs = swap(send)
    shard = join(own, theirs)
    hidden_theirs = swap(hidden)

    pieces = [shard]
    forward = backward = shard
    for _ in range(1, 4):
        forward = lax.ppermute(forward, "node", CW)
        backward = lax.ppermute(backward, "node", CCW)
        pieces += [forward, backward]
    pieces.append(lax.ppermute(forward, "node", CW))

    state = ()
    for k, piece in enumerate(pieces):
        state = add_term(k, order, piece, hidden, hidden_theirs, state)
    term, sent = state
    parts = lax.all_to_all(term.reshape(16, 64, units), ("x", "y"), 0, 0, tiled=True)
    theirs = swap(sent)
    grad_hidden = hidden_grads(order, core, pieces, theirs, w_down)
    keep, cross = plane_sums(zh, parts)
    far = lax.ppermute(cross, "zh", [(0, 1), (1, 0)])
    return grad_hidden, finish(keep, far)


def solution(mesh):
    fine = Mesh(mesh.devices.reshape(4, 2, 4, 2, 8), GRP + ("node",))
    return jax.shard_map(
        body,
        mesh=fine,
        in_specs=(P(GRP, "node"), P(GRP), P(GRP, "node"), P(None, "node"), P(GRP)),
        out_specs=(P(GRP, "node"), P(GRP, "node")),
        check_vma=False,
    )
```
